32 devices in a mesh: tm: 4 (over y, x), chan: 8 (over z, core).
Axes of the slice: x: 2, y: 2, z: 4, core: 2. Of those that a mesh axis runs over, the one named last changes fastest.
Arguments:
- voltages: bfloat16 [8, 4, 32768, 512], P(None, None, ('tm', 'chan')), may hold values from -6 to 6
- taps: float32 [4, 512], replicated, may hold values from -3 to 3
- busy_mask: int32 [512], replicated, may hold values from 0 to 1, as said below
- drift_low: int32 [512], replicated, may hold values from -16 to 1
Outputs:
- drift_power: float32 [8, 32, 16, 2048], P(None, 'chan', None, 'tm')
The draws below stay inside these ranges and needn't reach their ends.
Inputs may be any that keep to these rules, and one draw needn't show every extreme that they name: `busy_mask`: exactly 32 entries are 1.
All inputs are finite; a program needn't handle non-finite values.
Results may differ from the reference program's by a relative error of at most 0.008.
Values may be sent and summed in bfloat16 or wider, within the bound.
A program may use at most 192 MiB of HBM per device.

```python
import math
import jax
import jax.numpy as jnp
from jax import lax

COARSE_CHANNELS = 512
FINE = 2048
FA = 32
FB = 64
TAPS = 4
NDRIFT = 16
DSPAN = 16
FSTEP = 4
BEAMS = 8
SPEC = 32768
STEPS = 16
BUSY = 32
N_TM = 4


def draw_busy_mask(key, part):
    perm_key = jax.random.fold_in(key, 11)
    reward_key = jax.random.fold_in(key, 23)
    permuted_order = jax.random.permutation(perm_key, COARSE_CHANNELS).astype(jnp.int32)
    block_reward = jax.random.randint(reward_key, (COARSE_CHANNELS // 8,), 0, 4, dtype=jnp.int32)
    merit_scores = jnp.repeat(block_reward, 8, total_repeat_length=COARSE_CHANNELS) * (2 * COARSE_CHANNELS) + permuted_order
    chosen = lax.top_k(merit_scores, BUSY)[1]
    return jnp.zeros((COARSE_CHANNELS,), jnp.int32).at[chosen].set(1)


def set_ends(drawn, key, low, largest):
    longest = drawn.shape.index(max(drawn.shape))
    spots = []
    for shift in (0, 1):
        where = [jax.random.randint(jax.random.fold_in(key, axis), (), 0, length) for axis, length in enumerate(drawn.shape)]
        where[longest] = (where[longest] + shift) % drawn.shape[longest]
        spots.append(tuple(where))
    return drawn.at[spots[0]].set(low).at[spots[1]].set(largest)


def levels(own_key, extent, cuts, least, high):
    def one(axis_at, shards_of):
        draws = jax.random.uniform(jax.random.fold_in(jax.random.fold_in(own_key, 6), axis_at), (shards_of,), jnp.float32, least / len(cuts), high / len(cuts))
        return jnp.repeat(jnp.exp(draws), extent[axis_at] // shards_of).reshape((-1,) + (1,) * (len(extent) - axis_at - 1))

    factor_of = one(*cuts[0])
    for cut in cuts[1:]:
        factor_of = factor_of * one(*cut)
    return factor_of


def noise(key, dims, spread, most, shards=(), kind=jnp.bfloat16):
    level = levels(key, dims, shards, -0.22, 0.18) if shards else 1.0
    values = jax.random.normal(key, dims, jnp.float32) * spread * level
    return jnp.minimum(jnp.maximum(values, -most), most).astype(kind)


def setup_inputs(seed: int = 0) -> dict:
    keys = jax.random.split(jax.random.key(seed), 5)
    return {
        "voltages": noise(keys[0], (BEAMS, 4, SPEC, COARSE_CHANNELS), 1.0, 6.0, ((2, 32),)),
        "taps": noise(keys[1], (TAPS, COARSE_CHANNELS), 0.5, 3.0, (), jnp.float32),
        "busy_mask": draw_busy_mask(jax.random.fold_in(keys[4], 71), 0),
        "drift_low": set_ends(jax.random.randint(keys[3], (COARSE_CHANNELS,), -DSPAN, DSPAN - NDRIFT + 2), jax.random.fold_in(keys[3], 1), -DSPAN, (DSPAN - NDRIFT + 2) - 1).astype(jnp.int32),
    }


def busy_index(busy_mask, busy_count):
    mask_ints = busy_mask.astype(jnp.int32)
    before = (jnp.cumsum(mask_ints) - mask_ints).astype(jnp.int32)
    slot_ids = jnp.arange(busy_count, dtype=jnp.int32)
    is_slot = (mask_ints[:, None] == 1) & (before[:, None] == slot_ids[None, :])
    positions = jnp.arange(busy_mask.shape[0], dtype=jnp.int32)
    return jnp.sum(jnp.where(is_slot, positions[:, None], 0), axis=0).astype(jnp.int32)


def real_dft(sample_pos, freq_ids, length):
    phase_index = (sample_pos[:, None] * freq_ids[None, :]) % length
    angles = phase_index.astype(jnp.float32) * (2.0 * math.pi / length)
    cosines = jnp.cos(angles)
    sine_table = jnp.sin(angles)
    upper = jnp.stack([cosines, -sine_table], axis=1)
    lower = jnp.stack([sine_table, cosines], axis=1)
    return jnp.stack([upper, lower], axis=0).astype(jnp.bfloat16)


def to_bfloat(values):
    return lax.optimization_barrier(values.astype(jnp.bfloat16)).astype(jnp.float32)


def detect_power(spectra):
    items, lanes, chan_rows, samples = spectra.shape
    step_count = samples // (FA * FB)
    shaped = spectra.reshape(items, 2, 2, chan_rows, step_count, FA, FB).astype(jnp.float32)
    short_ids = jnp.arange(FA, dtype=jnp.int32)
    long_ids = jnp.arange(FB, dtype=jnp.int32)
    first_dft = real_dft(short_ids, short_ids, FA).astype(jnp.float32)
    second_dft = real_dft(long_ids, long_ids, FB).astype(jnp.float32)
    first_pass = jnp.einsum("xopctab,paqf->xoqctfb", shaped, first_dft, precision=lax.Precision.HIGHEST)
    twist = (short_ids[:, None] * long_ids[None, :]) % (FA * FB)
    twist_angles = twist.astype(jnp.float32) * (2.0 * math.pi / (FA * FB))
    twist_cos = jnp.cos(twist_angles)
    twist_sin = jnp.sin(twist_angles)
    real_part = first_pass[:, :, 0]
    imag_part = first_pass[:, :, 1]
    turned = jnp.stack([real_part * twist_cos + imag_part * twist_sin, imag_part * twist_cos - real_part * twist_sin], axis=2).astype(jnp.bfloat16)
    second_pass = jnp.einsum("xoqctfb,qbsg->xosctgf", turned.astype(jnp.float32), second_dft, precision=lax.Precision.HIGHEST)
    powers = jnp.sum(second_pass * second_pass, axis=(1, 2)) / (4.0 * FA * FB)
    return powers.reshape(items, chan_rows, step_count, FA * FB)


def drift_rows(step_rows, first_step, drift_rates, first_bin, bin_width, pad_width):
    padded = jnp.pad(step_rows, ((0, 0), (0, 0), (0, 0), (pad_width, pad_width)))
    chan_rows = step_rows.shape[1]
    chan_pick = jnp.arange(chan_rows, dtype=jnp.int32)[:, None, None]
    start_offsets = jnp.arange(bin_width, dtype=jnp.int32)
    running = jnp.zeros((step_rows.shape[0], chan_rows, drift_rates.shape[1], bin_width), jnp.float32)
    for row_index in range(step_rows.shape[2]):
        step_time = first_step + row_index
        anchor = pad_width + first_bin + drift_rates * step_time
        positions = (anchor[:, :, None] + start_offsets[None, None, :]).astype(jnp.int32)
        picked = padded[:, :, row_index][:, chan_pick, positions]
        running = running + picked
    return running


def reference(voltages, taps, busy_mask, drift_low):
    slot_index = busy_index(busy_mask, BUSY)
    coarse_dft = real_dft(jnp.arange(COARSE_CHANNELS, dtype=jnp.int32), slot_index, COARSE_CHANNELS).astype(jnp.float32)

    def one_beam(beam_volts):
        extended = jnp.pad(beam_volts, ((0, 0), (0, TAPS - 1), (0, 0)))
        filtered = taps[0] * extended[:, 0:SPEC]
        for tap_index in range(1, TAPS):
            filtered = filtered + taps[tap_index] * extended[:, tap_index:tap_index + SPEC]
        filtered = filtered.astype(jnp.bfloat16).astype(jnp.float32).reshape(2, 2, SPEC, COARSE_CHANNELS)
        coarse = jnp.einsum("opsn,pnqr->oqrs", filtered, coarse_dft, precision=lax.Precision.HIGHEST)
        coarse = (coarse * COARSE_CHANNELS ** -0.5).astype(jnp.bfloat16)
        return detect_power(coarse.reshape(1, 4, BUSY, SPEC))[0]

    powers = lax.map(one_beam, voltages)
    low_rates = drift_low[slot_index].astype(jnp.int32)
    drift_rates = (low_rates[:, None] + jnp.arange(NDRIFT, dtype=jnp.int32)[None, :]).astype(jnp.int32)
    pad_width = DSPAN * (STEPS - 1)
    drift_total = jnp.zeros((BEAMS, BUSY, NDRIFT, FINE), jnp.float32)
    for group_index in range(N_TM):
        step_rows = powers[:, :, group_index * FSTEP:(group_index + 1) * FSTEP]
        drift_total = drift_total + to_bfloat(drift_rows(step_rows, group_index * FSTEP, drift_rates, 0, FINE, pad_width))
    return drift_total / STEPS
```

```python
import math

import jax
import jax.numpy as jnp
import numpy as np
from jax import lax
from jax.experimental import pallas as pl
from jax.experimental.pallas import tpu as pltpu
from jax.sharding import PartitionSpec as P

FA = 32
FB = 64
TAPS = 4
NDRIFT = 16
DSPAN = 16
FSTEP = 4
CH_DEV = 1


def passed_along(block, axis, distance):
    devices = range(lax.axis_size(axis))
    route = [(i - distance, i) for i in devices if i - distance in devices]
    return lax.ppermute(block, axis, route)


def busy_index(busy_mask, busy_count):
    before = jnp.cumsum(busy_mask) - busy_mask
    slot_ids = jnp.arange(busy_count, dtype=jnp.int32)
    is_slot = (busy_mask[:, None] == 1) & (before[:, None] == slot_ids[None, :])
    positions = jnp.arange(busy_mask.shape[0], dtype=jnp.int32)
    return jnp.sum(jnp.where(is_slot, positions[:, None], 0), axis=0)


def real_dft(sample_pos, freq_ids, length):
    phase_index = sample_pos[:, None] * freq_ids[None, :] % length
    angles = phase_index.astype(jnp.float32) * (2.0 * math.pi / length)
    cosines = jnp.cos(angles)
    sine_table = jnp.sin(angles)
    upper = jnp.stack([cosines, -sine_table], axis=1)
    lower = jnp.stack([sine_table, cosines], axis=1)
    return jnp.stack([upper, lower], axis=0).astype(jnp.bfloat16)


def to_bfloat(values):
    return lax.optimization_barrier(values.astype(jnp.bfloat16)).astype(jnp.float32)


def detect_power(spectra):
    items, lanes, chan_rows, samples = spectra.shape
    step_count = samples // (FA * FB)
    shaped = spectra.reshape(items, 2, 2, chan_rows, step_count, FA, FB)
    short_ids = jnp.arange(FA, dtype=jnp.int32)
    long_ids = jnp.arange(FB, dtype=jnp.int32)
    first_pass = jnp.einsum(
        "xopctab,paqf->xoqctfb",
        shaped,
        real_dft(short_ids, short_ids, FA),
        preferred_element_type=jnp.float32,
    )
    twist = short_ids[:, None] * long_ids[None, :] % (FA * FB)
    twist_angles = twist.astype(jnp.float32) * (2.0 * math.pi / (FA * FB))
    twist_cos = jnp.cos(twist_angles)
    twist_sin = jnp.sin(twist_angles)
    real_part = first_pass[:, :, 0]
    imag_part = first_pass[:, :, 1]
    turned = jnp.stack(
        [
            real_part * twist_cos + imag_part * twist_sin,
            imag_part * twist_cos - real_part * twist_sin,
        ],
        axis=2,
    ).astype(jnp.bfloat16)
    second_pass = jnp.einsum(
        "xoqctfb,qbsg->xosctgf",
        turned,
        real_dft(long_ids, long_ids, FB),
        preferred_element_type=jnp.float32,
    )
    powers = jnp.sum(second_pass * second_pass, axis=(1, 2)) / (4.0 * FA * FB)
    return powers.reshape(items, chan_rows, step_count, FA * FB)


def drift_rows(step_rows, first_step, drift_rates, first_bin, bin_width, pad_width):
    padded = jnp.pad(step_rows, ((0, 0), (0, 0), (0, 0), (pad_width, pad_width)))
    chan_rows = step_rows.shape[1]
    rate_count = drift_rates.shape[1]
    running = jnp.zeros((step_rows.shape[0], chan_rows, rate_count, bin_width), jnp.float32)
    for row_index in range(step_rows.shape[2]):
        step_time = first_step + row_index
        power_row = padded[:, 0, row_index]
        windows = []
        for rate_pos in range(rate_count):
            start = pad_width + first_bin + drift_rates[0, rate_pos] * step_time
            windows.append(lax.dynamic_slice_in_dim(power_row, start, bin_width, 1))
        per_slot = [jnp.stack(windows, axis=1)]
        running = running + jnp.stack(per_slot, axis=1)
    return running


def slot_rates(slot_part, drift_low):
    one_hot = slot_part[:, None] == jnp.arange(drift_low.shape[0], dtype=jnp.int32)[None, :]
    low_rates = jnp.sum(jnp.where(one_hot, drift_low[None, :], 0), axis=1)
    return low_rates[:, None] + jnp.arange(NDRIFT, dtype=jnp.int32)[None, :]


def shards(voltages, taps, busy_mask, drift_low):
    tm_count = lax.axis_size("tm")
    chan_devices = lax.axis_size("chan")
    count_of_beams, lanes, spec_dev, chan_count = voltages.shape
    busy_count = CH_DEV * tm_count * chan_devices
    step_count = FSTEP * tm_count
    pad_width = DSPAN * (step_count - 1)
    slot_index = busy_index(busy_mask, busy_count)
    slot_order = (
        slot_index.reshape(chan_devices, tm_count, CH_DEV).transpose(1, 0, 2).reshape(busy_count)
    )
    coarse_dft = real_dft(jnp.arange(chan_count, dtype=jnp.int32), slot_order, chan_count)
    following = passed_along(voltages[:, :, : TAPS - 1], ("tm", "chan"), -1)
    extended = jnp.concatenate([voltages, following], axis=2)
    filtered = taps[0] * extended[:, :, 0:spec_dev]
    for tap_index in range(1, TAPS):
        filtered = filtered + taps[tap_index] * extended[:, :, tap_index : tap_index + spec_dev]
    filtered = filtered.astype(jnp.bfloat16).reshape(count_of_beams, 2, 2, spec_dev, chan_count)
    coarse = jnp.einsum(
        "bopsn,pnqr->boqrs", filtered, coarse_dft, preferred_element_type=jnp.float32
    )
    coarse = (
        (coarse * chan_count ** (-0.5))
        .astype(jnp.bfloat16)
        .reshape(count_of_beams, 4, busy_count, spec_dev)
    )
    arrived = lax.all_to_all(
        lax.all_to_all(coarse, "tm", split_axis=2, concat_axis=3, tiled=True),
        "chan",
        split_axis=2,
        concat_axis=3,
        tiled=True,
    )
    ordered = arrived.reshape(count_of_beams, 4, CH_DEV, chan_devices, tm_count, spec_dev)
    ordered = ordered.transpose(0, 1, 2, 4, 3, 5).reshape(
        count_of_beams, 4, CH_DEV, tm_count * chan_devices * spec_dev
    )
    powers = detect_power(ordered)
    first_slot = lax.axis_index("chan") * (CH_DEV * tm_count) + lax.axis_index("tm") * CH_DEV
    drift_rates = slot_rates(lax.dynamic_slice_in_dim(slot_index, first_slot, CH_DEV), drift_low)
    drift_total = jnp.zeros((count_of_beams, CH_DEV, NDRIFT, FA * FB), jnp.float32)
    for group_index in range(tm_count):
        step_rows = powers[:, :, group_index * FSTEP : (group_index + 1) * FSTEP]
        drift_total = drift_total + to_bfloat(
            drift_rows(step_rows, group_index * FSTEP, drift_rates, 0, FA * FB, pad_width)
        )
    result = lax.all_to_all(
        (drift_total / step_count).astype(jnp.bfloat16),
        "tm",
        split_axis=3,
        concat_axis=1,
        tiled=True,
    ).astype(jnp.float32)
    return result


LANES = 128
FINE = FA * FB
SHORT = FINE // LANES
SLOTS = 32
HALO_ROWS = 8
PAD = 256


def tap_weights(taps, busy_mask):
    chan_count = busy_mask.shape[0]
    ids = np.arange(chan_count)
    angles = (ids[:, None] * ids[None, :] % chan_count) * (2.0 * math.pi / chan_count)
    cos_table = jnp.asarray(np.cos(angles), jnp.bfloat16)
    sin_table = jnp.asarray(np.sin(angles), jnp.bfloat16)
    earlier = jnp.asarray(ids[None, :] < ids[:, None])
    before = jnp.sum(jnp.where(earlier, busy_mask[None, :], 0), axis=1)
    column = np.arange(2 * LANES)
    slot = jnp.asarray(column % SLOTS, jnp.int32)
    picked = ((busy_mask[:, None] == 1) & (before[:, None] == slot[None, :])).astype(jnp.bfloat16)
    cosines = jnp.dot(cos_table, picked, preferred_element_type=jnp.float32)
    sines = jnp.dot(sin_table, picked, preferred_element_type=jnp.float32)
    imag = jnp.asarray(column // 64 % 2 == 1)[None, :]
    upper = jnp.where(imag, -sines, cosines)
    lower = jnp.where(imag, cosines, sines)
    scaled = (taps * chan_count ** (-0.5)).T
    weights = []
    for pol in range(2):
        tap_of = 2 * (column // LANES) + (column // SLOTS % 2 ^ pol)
        factor = jnp.zeros((chan_count, 2 * LANES), jnp.float32)
        for tap in range(TAPS):
            factor = jnp.where(jnp.asarray(tap_of == tap)[None, :], scaled[:, tap : tap + 1], factor)
        weights += [(upper * factor).astype(jnp.bfloat16), (lower * factor).astype(jnp.bfloat16)]
    slot_low = lambda drift_low: jnp.sum(
        jnp.where(picked[:, :SLOTS] == 1, drift_low[:, None], 0), axis=0
    )
    return weights, slot_low


def coarse_kernel(first_ref, volt_ref, halo_ref, w00, w01, w10, w11, out_ref, g00, g01, g10, g11):
    rows = volt_ref.shape[2]
    chunk = min(rows, 256)
    for pol, (wa, wb, left, right) in enumerate(((w00, w01, g00, g01), (w10, w11, g10, g11))):
        for start in range(0, rows, chunk):
            part = jnp.dot(
                volt_ref[0, 2 * pol, start : start + chunk], wa[...], preferred_element_type=jnp.float32
            ) + jnp.dot(
                volt_ref[0, 2 * pol + 1, start : start + chunk], wb[...], preferred_element_type=jnp.float32
            )
            left[start : start + chunk] = part[:, :LANES]
            right[start : start + chunk] = part[:, LANES:]
        part = jnp.dot(
            halo_ref[0, 2 * pol], wa[...], preferred_element_type=jnp.float32
        ) + jnp.dot(halo_ref[0, 2 * pol + 1], wb[...], preferred_element_type=jnp.float32)
        left[rows : rows + HALO_ROWS] = part[:, :LANES]
        right[rows : rows + HALO_ROWS] = part[:, LANES:]
    count = rows // SHORT
    first_pol = lax.broadcasted_iota(jnp.int32, (count, LANES), 1) // SLOTS % 2 == 0

    def both(at):
        low = pl.ds(at, count, stride=SHORT)
        high = pl.ds(at + 2, count, stride=SHORT)
        return g00[low, :] + g01[high, :], g10[low, :] + g11[high, :]

    here = both(0)
    for at in range(SHORT):
        after = both(at + 1)
        value = jnp.where(
            first_pol,
            here[0] + pltpu.roll(after[0], LANES - SLOTS, 1),
            here[1] + pltpu.roll(after[1], SLOTS, 1),
        )
        out_ref[0, at * count : (at + 1) * count, :] = value.astype(jnp.bfloat16)
        here = after


def coarse_items(voltages, halo, weights, first, items):
    beams, lanes, rows, chan_count = voltages.shape
    whole = pl.BlockSpec((chan_count, 2 * LANES), lambda i, s: (0, 0))
    return pl.pallas_call(
        coarse_kernel,
        grid_spec=pltpu.PrefetchScalarGridSpec(
            num_scalar_prefetch=1,
            grid=(items,),
            in_specs=[
                pl.BlockSpec((1, lanes, rows, chan_count), lambda i, s: (s[0] + i, 0, 0, 0)),
                pl.BlockSpec((1, lanes, HALO_ROWS, chan_count), lambda i, s: (s[0] + i, 0, 0, 0)),
                whole,
                whole,
                whole,
                whole,
            ],
            out_specs=pl.BlockSpec((1, rows, LANES), lambda i, s: (i, 0, 0)),
            scratch_shapes=[pltpu.VMEM((rows + 3 * HALO_ROWS, LANES), jnp.float32)] * 4,
        ),
        out_shape=jax.ShapeDtypeStruct((items, rows, LANES), jnp.bfloat16),
        compiler_params=pltpu.CompilerParams(vmem_limit_bytes=48 * 2**20),
        cost_estimate=pl.CostEstimate(
            flops=items * lanes * rows * chan_count * 4 * LANES,
            bytes_accessed=items * lanes * rows * chan_count * 2,
            transcendentals=0,
        ),
    )(first.reshape(1), voltages, halo, *weights)


def short_dft(values, sign):
    count = len(values)
    if count == 1:
        return values
    even = short_dft(values[0::2], sign)
    odd = short_dft(values[1::2], sign)
    low, high = [], []
    for k in range(count // 2):
        term = odd[k]
        if k:
            flipped = pltpu.roll(term, LANES // 2, 1)
            angle = 2.0 * math.pi * k / count
            if 4 * k == count:
                term = flipped * sign
            else:
                term = term * math.cos(angle) + flipped * (sign * math.sin(angle))
        low.append(even[k] + term)
        high.append(even[k] - term)
    return low + high


def fine_kernel(core_ref, own_ref, other_ref, dft_ref, pick_ref, out_ref, mid, power):
    items, rows, _ = own_ref.shape
    count = rows // SHORT
    is_first = core_ref[0] == 0
    sign_of = lambda n: jnp.where(
        lax.broadcasted_iota(jnp.int32, (n, LANES), 1) < LANES // 2, 1.0, -1.0
    ).astype(jnp.float32)
    sign_full = sign_of(2 * count)
    for at in range(SHORT):
        plain, flipped = [], []
        for item in range(items):
            own = own_ref[item, at * count : (at + 1) * count, :]
            other = other_ref[item, at * count : (at + 1) * count, :]
            block = jnp.concatenate(
                [jnp.where(is_first, own, other), jnp.where(is_first, other, own)], axis=0
            )
            plain.append(block)
            swapped = pltpu.roll(block.astype(jnp.float32), LANES // 2, 1) * sign_full
            flipped.append(swapped.astype(jnp.bfloat16))
        stacked = jnp.concatenate(
            [jnp.concatenate(plain, axis=1), jnp.concatenate(flipped, axis=1)], axis=0
        )
        mid[at] = jnp.dot(dft_ref[at], stacked, preferred_element_type=jnp.float32)
    step = 16
    sign = sign_of(step)
    for item in range(items):
        lanes = pl.ds(item * LANES, LANES)

        @pl.loop(0, LANES // step)
        def _(block):
            at_row = pl.multiple_of(block * step, step)
            spectra = short_dft([mid[at, pl.ds(at_row, step), lanes] for at in range(SHORT)], sign)
            for high, value in enumerate(spectra):
                where = pl.ds(pl.multiple_of(high * LANES + at_row, step), step)
                power[where, lanes] = (value * value).astype(jnp.bfloat16)

    width = 512
    for start in range(0, SHORT * LANES, width):
        out_ref[:, start : start + width] = lax.dot_general(
            pick_ref[...],
            power[start : start + width, :],
            (((1,), (1,)), ((), ())),
            preferred_element_type=jnp.float32,
        ).astype(jnp.bfloat16)


def fine_powers(own, other, core, groups):
    items, rows, _ = own.shape
    position = np.arange(SHORT)[:, None, None] + SHORT * np.arange(LANES)[None, None, :]
    angles = (position * np.arange(LANES)[None, :, None] % FINE) * (2.0 * math.pi / FINE)
    dft = jnp.asarray(np.concatenate([np.cos(angles), np.sin(angles)], axis=2), jnp.bfloat16)
    per_group = SLOTS // groups
    row = np.arange(SLOTS * items)
    row_group, row_slot, row_item = row // (per_group * items), row // items % per_group, row % items
    lane = np.arange(items * LANES)
    pick = (row_item[:, None] == lane[None, :] // LANES) & (
        (row_group * per_group + row_slot)[:, None] == lane[None, :] % SLOTS
    )
    vmem = pl.BlockSpec(memory_space=pltpu.VMEM)
    return pl.pallas_call(
        fine_kernel,
        in_specs=[pl.BlockSpec(memory_space=pltpu.SMEM), vmem, vmem, vmem, vmem],
        out_specs=vmem,
        out_shape=jax.ShapeDtypeStruct((SLOTS * items, FINE), jnp.bfloat16),
        scratch_shapes=[
            pltpu.VMEM((SHORT, LANES, items * LANES), jnp.float32),
            pltpu.VMEM((FINE, items * LANES), jnp.bfloat16),
        ],
        compiler_params=pltpu.CompilerParams(vmem_limit_bytes=48 * 2**20),
        cost_estimate=pl.CostEstimate(flops=2 * 10**9, bytes_accessed=4 * 10**6, transcendentals=0),
    )(core.reshape(1), own, other, dft, jnp.asarray(pick, jnp.bfloat16))


def drift_kernel(scale, low_ref, in_ref, out_ref, rows_ref):
    steps, cores, _, window = in_ref.shape
    beams, slots, rates, width = out_ref.shape
    items = beams // cores
    for t in range(steps):
        halves = [in_ref[t, core].astype(jnp.float32) for core in range(cores)]
        for slot in range(slots):
            rows_ref[slot, t] = jnp.concatenate(
                [half[slot * items : (slot + 1) * items] for half in halves], axis=0
            )
    lane = lax.broadcasted_iota(jnp.int32, (beams, LANES), 1)
    tiles = width // LANES
    for slot in range(slots):
        low = low_ref[slot]
        for rate in range(rates):
            totals = [jnp.zeros((beams, LANES), jnp.float32)] * tiles
            for t in range(steps):
                start = (low + rate) * t + PAD
                rest = lax.rem(start, LANES)
                base = start - rest
                turned = []
                for tile in range(tiles + 1):
                    at = pl.ds(pl.multiple_of(base + tile * LANES, LANES), LANES)
                    turned.append(rows_ref[slot, t, :, at])
                if t:
                    back = LANES - rest
                    turned = [pltpu.roll(part, back, 1) for part in turned]
                    keep = lane < back
                    turned = [jnp.where(keep, turned[k], turned[k + 1]) for k in range(tiles)]
                totals = [total + part for total, part in zip(totals, turned)]
            out_ref[:, slot, rate, :] = jnp.concatenate(totals, axis=1) * scale


def drift_sums(rows, low_rates, beams, width):
    steps = rows.shape[0]
    slots = low_rates.shape[0]
    vmem = pl.BlockSpec(memory_space=pltpu.VMEM)
    kernel = lambda *refs: drift_kernel(1.0 / (4.0 * FINE * steps), *refs)
    return pl.pallas_call(
        kernel,
        in_specs=[pl.BlockSpec(memory_space=pltpu.SMEM), vmem],
        out_specs=vmem,
        out_shape=jax.ShapeDtypeStruct((beams, slots, NDRIFT, width), jnp.float32),
        scratch_shapes=[pltpu.VMEM((slots, steps, beams, rows.shape[3]), jnp.float32)],
        compiler_params=pltpu.CompilerParams(vmem_limit_bytes=48 * 2**20),
    )(low_rates, rows)


def paired_shards(voltages, taps, busy_mask, drift_low):
    tm_count = lax.axis_size("tm")
    chan_devices = lax.axis_size("chan")
    beams, lanes, rows, chan_count = voltages.shape
    items = beams // 2
    slots = SLOTS // chan_devices
    chan = lax.axis_index("chan")
    core = lax.rem(chan, 2)
    halo = passed_along(voltages[:, :, :HALO_ROWS], ("tm", "chan"), -1)
    weights, slot_low = tap_weights(taps, busy_mask)
    low_rates = lax.dynamic_slice_in_dim(slot_low(drift_low), chan * slots, slots)
    sent = coarse_items(voltages, halo, weights, (1 - core) * items, items)
    other = lax.ppermute(sent, "chan", [(i, i ^ 1) for i in range(chan_devices)])
    own = coarse_items(voltages, halo, weights, core * items, items)
    powers = fine_powers(own, other, core, chan_devices)
    powers = powers.reshape(chan_devices, slots * items, FINE)
    group = lax.all_to_all(powers, "chan", split_axis=0, concat_axis=0, tiled=True)
    width = FINE // tm_count
    padded = jnp.pad(group, ((0, 0), (0, 0), (PAD, PAD)))
    windows = jnp.stack(
        [padded[:, :, m * width : (m + 1) * width + 2 * PAD] for m in range(tm_count)], axis=0
    )
    arrived = lax.all_to_all(windows, "tm", split_axis=0, concat_axis=0, tiled=True)
    arrived = arrived.reshape(
        tm_count * chan_devices // 2, 2, slots * items, width + 2 * PAD
    )
    return drift_sums(arrived, low_rates, beams, width)


def two_devices_hold_a_step(mesh, voltages):
    tm_count, chan_devices = mesh.shape["tm"], mesh.shape["chan"]
    rows = voltages.shape[2] // (tm_count * chan_devices)
    return (
        2 * rows == FINE
        and chan_devices == 2 * FSTEP
        and CH_DEV * tm_count * chan_devices == SLOTS
        and voltages.shape[0] == 8
        and PAD >= DSPAN * (FSTEP * tm_count - 1)
        and FINE // tm_count % LANES == 0
    )


def solution(mesh):
    in_specs = (P(None, None, ("tm", "chan"), None), P(), P(), P())
    out_specs = P(None, "chan", None, "tm")

    def run(voltages, taps, busy_mask, drift_low):
        body = paired_shards if two_devices_hold_a_step(mesh, voltages) else shards
        return jax.shard_map(
            body, mesh=mesh, in_specs=in_specs, out_specs=out_specs, check_vma=False
        )(voltages, taps, busy_mask, drift_low)

    return run
```

```python
import math

import jax
import jax.numpy as jnp
import numpy as np
from jax import lax
from jax.experimental import pallas as pl
from jax.experimental.pallas import tpu as pltpu
from jax.sharding import PartitionSpec as P

FA = 32
FB = 64
TAPS = 4
NDRIFT = 16
DSPAN = 16
FSTEP = 4
CH_DEV = 1


def passed_along(block, axis, distance):
    devices = range(lax.axis_size(axis))
    route = [(i - distance, i) for i in devices if i - distance in devices]
    return lax.ppermute(block, axis, route)


def busy_index(busy_mask, busy_count):
    before = jnp.cumsum(busy_mask) - busy_mask
    slot_ids = jnp.arange(busy_count, dtype=jnp.int32)
    is_slot = (busy_mask[:, None] == 1) & (before[:, None] == slot_ids[None, :])
    positions = jnp.arange(busy_mask.shape[0], dtype=jnp.int32)
    return jnp.sum(jnp.where(is_slot, positions[:, None], 0), axis=0)


def real_dft(sample_pos, freq_ids, length):
    phase_index = sample_pos[:, None] * freq_ids[None, :] % length
    angles = phase_index.astype(jnp.float32) * (2.0 * math.pi / length)
    cosines = jnp.cos(angles)
    sine_table = jnp.sin(angles)
    upper = jnp.stack([cosines, -sine_table], axis=1)
    lower = jnp.stack([sine_table, cosines], axis=1)
    return jnp.stack([upper, lower], axis=0).astype(jnp.bfloat16)


def to_bfloat(values):
    return lax.optimization_barrier(values.astype(jnp.bfloat16)).astype(jnp.float32)


def detect_power(spectra):
    items, lanes, chan_rows, samples = spectra.shape
    step_count = samples // (FA * FB)
    shaped = spectra.reshape(items, 2, 2, chan_rows, step_count, FA, FB)
    short_ids = jnp.arange(FA, dtype=jnp.int32)
    long_ids = jnp.arange(FB, dtype=jnp.int32)
    first_pass = jnp.einsum(
        "xopctab,paqf->xoqctfb",
        shaped,
        real_dft(short_ids, short_ids, FA),
        preferred_element_type=jnp.float32,
    )
    twist = short_ids[:, None] * long_ids[None, :] % (FA * FB)
    twist_angles = twist.astype(jnp.float32) * (2.0 * math.pi / (FA * FB))
    twist_cos = jnp.cos(twist_angles)
    twist_sin = jnp.sin(twist_angles)
    real_part = first_pass[:, :, 0]
    imag_part = first_pass[:, :, 1]
    turned = jnp.stack(
        [
            real_part * twist_cos + imag_part * twist_sin,
            imag_part * twist_cos - real_part * twist_sin,
        ],
        axis=2,
    ).astype(jnp.bfloat16)
    second_pass = jnp.einsum(
        "xoqctfb,qbsg->xosctgf",
        turned,
        real_dft(long_ids, long_ids, FB),
        preferred_element_type=jnp.float32,
    )
    powers = jnp.sum(second_pass * second_pass, axis=(1, 2)) / (4.0 * FA * FB)
    return powers.reshape(items, chan_rows, step_count, FA * FB)


def drift_rows(step_rows, first_step, drift_rates, first_bin, bin_width, pad_width):
    padded = jnp.pad(step_rows, ((0, 0), (0, 0), (0, 0), (pad_width, pad_width)))
    chan_rows = step_rows.shape[1]
    rate_count = drift_rates.shape[1]
    running = jnp.zeros((step_rows.shape[0], chan_rows, rate_count, bin_width), jnp.float32)
    for row_index in range(step_rows.shape[2]):
        step_time = first_step + row_index
        power_row = padded[:, 0, row_index]
        windows = []
        for rate_pos in range(rate_count):
            start = pad_width + first_bin + drift_rates[0, rate_pos] * step_time
            windows.append(lax.dynamic_slice_in_dim(power_row, start, bin_width, 1))
        per_slot = [jnp.stack(windows, axis=1)]
        running = running + jnp.stack(per_slot, axis=1)
    return running


def slot_rates(slot_part, drift_low):
    one_hot = slot_part[:, None] == jnp.arange(drift_low.shape[0], dtype=jnp.int32)[None, :]
    low_rates = jnp.sum(jnp.where(one_hot, drift_low[None, :], 0), axis=1)
    return low_rates[:, None] + jnp.arange(NDRIFT, dtype=jnp.int32)[None, :]


def shards(voltages, taps, busy_mask, drift_low):
    tm_count = lax.axis_size("tm")
    chan_devices = lax.axis_size("chan")
    count_of_beams, lanes, spec_dev, chan_count = voltages.shape
    busy_count = CH_DEV * tm_count * chan_devices
    step_count = FSTEP * tm_count
    pad_width = DSPAN * (step_count - 1)
    slot_index = busy_index(busy_mask, busy_count)
    slot_order = (
        slot_index.reshape(chan_devices, tm_count, CH_DEV).transpose(1, 0, 2).reshape(busy_count)
    )
    coarse_dft = real_dft(jnp.arange(chan_count, dtype=jnp.int32), slot_order, chan_count)
    following = passed_along(voltages[:, :, : TAPS - 1], ("tm", "chan"), -1)
    extended = jnp.concatenate([voltages, following], axis=2)
    filtered = taps[0] * extended[:, :, 0:spec_dev]
    for tap_index in range(1, TAPS):
        filtered = filtered + taps[tap_index] * extended[:, :, tap_index : tap_index + spec_dev]
    filtered = filtered.astype(jnp.bfloat16).reshape(count_of_beams, 2, 2, spec_dev, chan_count)
    coarse = jnp.einsum(
        "bopsn,pnqr->boqrs", filtered, coarse_dft, preferred_element_type=jnp.float32
    )
    coarse = (
        (coarse * chan_count ** (-0.5))
        .astype(jnp.bfloat16)
        .reshape(count_of_beams, 4, busy_count, spec_dev)
    )
    arrived = lax.all_to_all(
        lax.all_to_all(coarse, "tm", split_axis=2, concat_axis=3, tiled=True),
        "chan",
        split_axis=2,
        concat_axis=3,
        tiled=True,
    )
    ordered = arrived.reshape(count_of_beams, 4, CH_DEV, chan_devices, tm_count, spec_dev)
    ordered = ordered.transpose(0, 1, 2, 4, 3, 5).reshape(
        count_of_beams, 4, CH_DEV, tm_count * chan_devices * spec_dev
    )
    powers = detect_power(ordered)
    first_slot = lax.axis_index("chan") * (CH_DEV * tm_count) + lax.axis_index("tm") * CH_DEV
    drift_rates = slot_rates(lax.dynamic_slice_in_dim(slot_index, first_slot, CH_DEV), drift_low)
    drift_total = jnp.zeros((count_of_beams, CH_DEV, NDRIFT, FA * FB), jnp.float32)
    for group_index in range(tm_count):
        step_rows = powers[:, :, group_index * FSTEP : (group_index + 1) * FSTEP]
        drift_total = drift_total + to_bfloat(
            drift_rows(step_rows, group_index * FSTEP, drift_rates, 0, FA * FB, pad_width)
        )
    result = lax.all_to_all(
        (drift_total / step_count).astype(jnp.bfloat16),
        "tm",
        split_axis=3,
        concat_axis=1,
        tiled=True,
    ).astype(jnp.float32)
    return result


LANES = 128
FINE = FA * FB
SHORT = FINE // LANES
SLOTS = 32
HALO_ROWS = 8
PAD = 256


def tap_weights(taps, busy_mask):
    chan_count = busy_mask.shape[0]
    ids = np.arange(chan_count)
    angles = (ids[:, None] * ids[None, :] % chan_count) * (2.0 * math.pi / chan_count)
    cos_table = jnp.asarray(np.cos(angles), jnp.bfloat16)
    sin_table = jnp.asarray(np.sin(angles), jnp.bfloat16)
    earlier = jnp.asarray(ids[None, :] < ids[:, None])
    before = jnp.sum(jnp.where(earlier, busy_mask[None, :], 0), axis=1)
    column = np.arange(2 * LANES)
    slot = jnp.asarray(column % SLOTS, jnp.int32)
    picked = ((busy_mask[:, None] == 1) & (before[:, None] == slot[None, :])).astype(jnp.bfloat16)
    cosines = jnp.dot(cos_table, picked, preferred_element_type=jnp.float32)
    sines = jnp.dot(sin_table, picked, preferred_element_type=jnp.float32)
    imag = jnp.asarray(column // 64 % 2 == 1)[None, :]
    upper = jnp.where(imag, -sines, cosines)
    lower = jnp.where(imag, cosines, sines)
    scaled = (taps * chan_count ** (-0.5)).T
    weights = []
    for pol in range(2):
        tap_of = 2 * (column // LANES) + (column // SLOTS % 2 ^ pol)
        factor = jnp.zeros((chan_count, 2 * LANES), jnp.float32)
        for tap in range(TAPS):
            factor = jnp.where(jnp.asarray(tap_of == tap)[None, :], scaled[:, tap : tap + 1], factor)
        weights += [(upper * factor).astype(jnp.bfloat16), (lower * factor).astype(jnp.bfloat16)]
    slot_low = lambda drift_low: jnp.sum(
        jnp.where(picked[:, :SLOTS] == 1, drift_low[:, None], 0), axis=0
    )
    return weights, slot_low


def coarse_kernel(first_ref, volt_ref, halo_ref, w00, w01, w10, w11, out_ref, g00, g01, g10, g11):
    rows = volt_ref.shape[2]
    chunk = min(rows, 256)
    for pol, (wa, wb, left, right) in enumerate(((w00, w01, g00, g01), (w10, w11, g10, g11))):
        for start in range(0, rows, chunk):
            part = jnp.dot(
                volt_ref[0, 2 * pol, start : start + chunk], wa[...], preferred_element_type=jnp.float32
            ) + jnp.dot(
                volt_ref[0, 2 * pol + 1, start : start + chunk], wb[...], preferred_element_type=jnp.float32
            )
            left[start : start + chunk] = part[:, :LANES]
            right[start : start + chunk] = part[:, LANES:]
        part = jnp.dot(
            halo_ref[0, 2 * pol], wa[...], preferred_element_type=jnp.float32
        ) + jnp.dot(halo_ref[0, 2 * pol + 1], wb[...], preferred_element_type=jnp.float32)
        left[rows : rows + HALO_ROWS] = part[:, :LANES]
        right[rows : rows + HALO_ROWS] = part[:, LANES:]
    count = rows // SHORT
    first_pol = lax.broadcasted_iota(jnp.int32, (count, LANES), 1) // SLOTS % 2 == 0

    def both(at):
        low = pl.ds(at, count, stride=SHORT)
        high = pl.ds(at + 2, count, stride=SHORT)
        return g00[low, :] + g01[high, :], g10[low, :] + g11[high, :]

    here = both(0)
    for at in range(SHORT):
        after = both(at + 1)
        value = jnp.where(
            first_pol,
            here[0] + pltpu.roll(after[0], LANES - SLOTS, 1),
            here[1] + pltpu.roll(after[1], SLOTS, 1),
        )
        out_ref[0, at * count : (at + 1) * count, :] = value.astype(jnp.bfloat16)
        here = after


def coarse_items(voltages, halo, weights, first, items):
    beams, lanes, rows, chan_count = voltages.shape
    whole = pl.BlockSpec((chan_count, 2 * LANES), lambda i, s: (0, 0))
    return pl.pallas_call(
        coarse_kernel,
        grid_spec=pltpu.PrefetchScalarGridSpec(
            num_scalar_prefetch=1,
            grid=(items,),
            in_specs=[
                pl.BlockSpec((1, lanes, rows, chan_count), lambda i, s: (s[0] + i, 0, 0, 0)),
                pl.BlockSpec((1, lanes, HALO_ROWS, chan_count), lambda i, s: (s[0] + i, 0, 0, 0)),
                whole,
                whole,
                whole,
                whole,
            ],
            out_specs=pl.BlockSpec((1, rows, LANES), lambda i, s: (i, 0, 0)),
            scratch_shapes=[pltpu.VMEM((rows + 3 * HALO_ROWS, LANES), jnp.float32)] * 4,
        ),
        out_shape=jax.ShapeDtypeStruct((items, rows, LANES), jnp.bfloat16),
        compiler_params=pltpu.CompilerParams(vmem_limit_bytes=48 * 2**20),
        cost_estimate=pl.CostEstimate(
            flops=items * lanes * rows * chan_count * 4 * LANES,
            bytes_accessed=items * lanes * rows * chan_count * 2,
            transcendentals=0,
        ),
    )(first.reshape(1), voltages, halo, *weights)


def short_dft(values, sign):
    count = len(values)
    if count == 1:
        return values
    even = short_dft(values[0::2], sign)
    odd = short_dft(values[1::2], sign)
    low, high = [], []
    for k in range(count // 2):
        term = odd[k]
        if k:
            flipped = pltpu.roll(term, LANES // 2, 1)
            angle = 2.0 * math.pi * k / count
            if 4 * k == count:
                term = flipped * sign
            else:
                term = term * math.cos(angle) + flipped * (sign * math.sin(angle))
        low.append(even[k] + term)
        high.append(even[k] - term)
    return low + high


def fine_kernel(core_ref, own_ref, other_ref, dft_ref, pick_ref, out_ref, mid, power):
    items, rows, _ = own_ref.shape
    count = rows // SHORT
    is_first = core_ref[0] == 0
    sign_of = lambda n: jnp.where(
        lax.broadcasted_iota(jnp.int32, (n, LANES), 1) < LANES // 2, 1.0, -1.0
    ).astype(jnp.float32)
    sign_full = sign_of(2 * count)
    for at in range(SHORT):
        plain, flipped = [], []
        for item in range(items):
            own = own_ref[item, at * count : (at + 1) * count, :]
            other = other_ref[item, at * count : (at + 1) * count, :]
            block = jnp.concatenate(
                [jnp.where(is_first, own, other), jnp.where(is_first, other, own)], axis=0
            )
            plain.append(block)
            swapped = pltpu.roll(block.astype(jnp.float32), LANES // 2, 1) * sign_full
            flipped.append(swapped.astype(jnp.bfloat16))
        stacked = jnp.concatenate(
            [jnp.concatenate(plain, axis=1), jnp.concatenate(flipped, axis=1)], axis=0
        )
        mid[at] = jnp.dot(dft_ref[at], stacked, preferred_element_type=jnp.float32)
    step = 16
    sign = sign_of(step)
    for item in range(items):
        lanes = pl.ds(item * LANES, LANES)

        @pl.loop(0, LANES // step)
        def _(block):
            at_row = pl.multiple_of(block * step, step)
            spectra = short_dft([mid[at, pl.ds(at_row, step), lanes] for at in range(SHORT)], sign)
            for high, value in enumerate(spectra):
                where = pl.ds(pl.multiple_of(high * LANES + at_row, step), step)
                power[where, lanes] = (value * value).astype(jnp.bfloat16)

    width = 512
    for start in range(0, SHORT * LANES, width):
        out_ref[:, start : start + width] = lax.dot_general(
            pick_ref[...],
            power[start : start + width, :],
            (((1,), (1,)), ((), ())),
            preferred_element_type=jnp.float32,
        ).astype(jnp.bfloat16)


def fine_powers(own, other, core, groups):
    items, rows, _ = own.shape
    position = np.arange(SHORT)[:, None, None] + SHORT * np.arange(LANES)[None, None, :]
    angles = (position * np.arange(LANES)[None, :, None] % FINE) * (2.0 * math.pi / FINE)
    dft = jnp.asarray(np.concatenate([np.cos(angles), np.sin(angles)], axis=2), jnp.bfloat16)
    per_group = SLOTS // groups
    row = np.arange(SLOTS * items)
    row_group, row_slot, row_item = row // (per_group * items), row // items % per_group, row % items
    lane = np.arange(items * LANES)
    pick = (row_item[:, None] == lane[None, :] // LANES) & (
        (row_group * per_group + row_slot)[:, None] == lane[None, :] % SLOTS
    )
    vmem = pl.BlockSpec(memory_space=pltpu.VMEM)
    return pl.pallas_call(
        fine_kernel,
        in_specs=[pl.BlockSpec(memory_space=pltpu.SMEM), vmem, vmem, vmem, vmem],
        out_specs=vmem,
        out_shape=jax.ShapeDtypeStruct((SLOTS * items, FINE), jnp.bfloat16),
        scratch_shapes=[
            pltpu.VMEM((SHORT, LANES, items * LANES), jnp.float32),
            pltpu.VMEM((FINE, items * LANES), jnp.bfloat16),
        ],
        compiler_params=pltpu.CompilerParams(vmem_limit_bytes=48 * 2**20),
        cost_estimate=pl.CostEstimate(flops=2 * 10**9, bytes_accessed=4 * 10**6, transcendentals=0),
    )(core.reshape(1), own, other, dft, jnp.asarray(pick, jnp.bfloat16))


def window_start(part, width):
    return jnp.clip(part * width - PAD, 0, FINE - (width + 2 * PAD))


def exchange_kernel(tm_count, chan_devices, in_ref, out_ref, held, sent1, came1, sent2, came2, local):
    tm, chan = lax.axis_index("tm"), lax.axis_index("chan")
    window = out_ref.shape[3]
    width = FINE // tm_count
    MESH = pl.DeviceIdType.MESH
    tm_peers = [lax.rem(tm + q, tm_count) for q in range(tm_count)]
    chan_peers = [lax.rem(chan + k, chan_devices) for k in range(chan_devices)]
    chan_from = [lax.rem(chan + chan_devices - k, chan_devices) for k in range(chan_devices)]
    tm_from = [lax.rem(tm + tm_count - q, tm_count) for q in range(tm_count)]
    barrier = pltpu.get_barrier_semaphore()
    for q in range(1, tm_count):
        pl.semaphore_signal(barrier, inc=1, device_id=(tm_peers[q], chan), device_id_type=MESH)
    for k in range(1, chan_devices):
        pl.semaphore_signal(barrier, inc=1, device_id=(tm, chan_peers[k]), device_id_type=MESH)
    pl.semaphore_wait(barrier, tm_count + chan_devices - 2)

    first = []
    for k in range(1, chan_devices):
        copy = pltpu.make_async_remote_copy(
            src_ref=in_ref.at[chan_peers[k]],
            dst_ref=held.at[k],
            send_sem=sent1.at[k],
            recv_sem=came1.at[k],
            device_id=(tm, chan_peers[k]),
            device_id_type=MESH,
        )
        copy.start()
        first.append(copy)
    second, near = [], []
    for k in range(chan_devices):
        if k:
            first[k - 1].wait_recv()
        block = held.at[k] if k else in_ref.at[chan]
        for q in range(1, tm_count):
            start = pl.multiple_of(window_start(tm_peers[q], width), LANES)
            copy = pltpu.make_async_remote_copy(
                src_ref=block.at[:, pl.ds(start, window)],
                dst_ref=out_ref.at[tm, chan_from[k]],
                send_sem=sent2.at[k, q],
                recv_sem=came2.at[k, q],
                device_id=(tm_peers[q], chan),
                device_id_type=MESH,
            )
            copy.start()
            second.append(copy)
        start = pl.multiple_of(window_start(tm, width), LANES)
        copy = pltpu.make_async_copy(
            block.at[:, pl.ds(start, window)], out_ref.at[tm, chan_from[k]], local.at[k]
        )
        copy.start()
        near.append(copy)
    for copy in first + second:
        copy.wait_send()
    for copy in near:
        copy.wait()
    for k in range(chan_devices):
        for q in range(1, tm_count):
            pltpu.make_async_remote_copy(
                src_ref=held.at[k, :, pl.ds(0, window)],
                dst_ref=out_ref.at[tm_from[q], chan_from[k]],
                send_sem=sent2.at[k, q],
                recv_sem=came2.at[k, q],
                device_id=(tm_peers[q], chan),
                device_id_type=MESH,
            ).wait_recv()


def exchange(powers, tm_count, chan_devices):
    rows = powers.shape[1]
    window = FINE // tm_count + 2 * PAD
    vmem = pl.BlockSpec(memory_space=pltpu.VMEM)
    kernel = lambda *refs: exchange_kernel(tm_count, chan_devices, *refs)
    dma = pltpu.SemaphoreType.DMA
    return pl.pallas_call(
        kernel,
        in_specs=[vmem],
        out_specs=vmem,
        out_shape=jax.ShapeDtypeStruct((tm_count, chan_devices, rows, window), jnp.bfloat16),
        scratch_shapes=[
            pltpu.VMEM(powers.shape, jnp.bfloat16),
            dma((chan_devices,)),
            dma((chan_devices,)),
            dma((chan_devices, tm_count)),
            dma((chan_devices, tm_count)),
            dma((chan_devices,)),
        ],
        compiler_params=pltpu.CompilerParams(collective_id=0, has_side_effects=True),
    )(powers)


def drift_kernel(scale, low_ref, in_ref, out_ref, rows_ref):
    steps, cores, _, window = in_ref.shape
    beams, slots, rates, width = out_ref.shape
    items = beams // cores
    edge = jnp.zeros(rows_ref.shape[:3] + (PAD,), jnp.float32)
    rows_ref[:, :, :, :PAD] = edge
    rows_ref[:, :, :, PAD + window :] = edge
    offset = low_ref[slots]
    for t in range(steps):
        halves = [in_ref[t, core].astype(jnp.float32) for core in range(cores)]
        for slot in range(slots):
            rows_ref[slot, t, :, PAD : PAD + window] = jnp.concatenate(
                [half[slot * items : (slot + 1) * items] for half in halves], axis=0
            )
    lane = lax.broadcasted_iota(jnp.int32, (beams, LANES), 1)
    tiles = width // LANES
    for slot in range(slots):
        low = low_ref[slot]
        for rate in range(rates):
            totals = [jnp.zeros((beams, LANES), jnp.float32)] * tiles
            for t in range(steps):
                start = (low + rate) * t + PAD + offset
                rest = lax.rem(start, LANES)
                base = start - rest
                turned = []
                for tile in range(tiles + 1):
                    at = pl.ds(pl.multiple_of(base + tile * LANES, LANES), LANES)
                    turned.append(rows_ref[slot, t, :, at])
                if t:
                    back = LANES - rest
                    turned = [pltpu.roll(part, back, 1) for part in turned]
                    keep = lane < back
                    turned = [jnp.where(keep, turned[k], turned[k + 1]) for k in range(tiles)]
                totals = [total + part for total, part in zip(totals, turned)]
            out_ref[:, slot, rate, :] = jnp.concatenate(totals, axis=1) * scale


def drift_sums(rows, low_rates, offset, beams, width):
    steps = rows.shape[0]
    slots = low_rates.shape[0]
    vmem = pl.BlockSpec(memory_space=pltpu.VMEM)
    kernel = lambda *refs: drift_kernel(1.0 / (4.0 * FINE * steps), *refs)
    return pl.pallas_call(
        kernel,
        in_specs=[pl.BlockSpec(memory_space=pltpu.SMEM), vmem],
        out_specs=vmem,
        out_shape=jax.ShapeDtypeStruct((beams, slots, NDRIFT, width), jnp.float32),
        scratch_shapes=[pltpu.VMEM((slots, steps, beams, rows.shape[3] + 2 * PAD), jnp.float32)],
        compiler_params=pltpu.CompilerParams(vmem_limit_bytes=48 * 2**20),
    )(jnp.concatenate([low_rates, offset[None]]), rows)


def paired_shards(voltages, taps, busy_mask, drift_low):
    tm_count = lax.axis_size("tm")
    chan_devices = lax.axis_size("chan")
    beams, lanes, rows, chan_count = voltages.shape
    items = beams // 2
    slots = SLOTS // chan_devices
    chan = lax.axis_index("chan")
    core = lax.rem(chan, 2)
    halo = passed_along(voltages[:, :, :HALO_ROWS], ("tm", "chan"), -1)
    weights, slot_low = tap_weights(taps, busy_mask)
    low_rates = lax.dynamic_slice_in_dim(slot_low(drift_low), chan * slots, slots)
    sent = coarse_items(voltages, halo, weights, (1 - core) * items, items)
    other = lax.ppermute(sent, "chan", [(i, i ^ 1) for i in range(chan_devices)])
    own = coarse_items(voltages, halo, weights, core * items, items)
    powers = fine_powers(own, other, core, chan_devices)
    powers = powers.reshape(chan_devices, slots * items, FINE)
    width = FINE // tm_count
    arrived = exchange(powers, tm_count, chan_devices).reshape(
        tm_count * chan_devices // 2, 2, slots * items, width + 2 * PAD
    )
    tm = lax.axis_index("tm")
    offset = tm * width - window_start(tm, width)
    return drift_sums(arrived, low_rates, offset, beams, width)


def two_devices_hold_a_step(mesh, voltages):
    tm_count, chan_devices = mesh.shape["tm"], mesh.shape["chan"]
    rows = voltages.shape[2] // (tm_count * chan_devices)
    return (
        2 * rows == FINE
        and chan_devices == 2 * FSTEP
        and CH_DEV * tm_count * chan_devices == SLOTS
        and voltages.shape[0] == 8
        and PAD >= DSPAN * (FSTEP * tm_count - 1)
        and FINE // tm_count % PAD == 0
        and FINE // tm_count + 2 * PAD <= FINE
    )


def solution(mesh):
    in_specs = (P(None, None, ("tm", "chan"), None), P(), P(), P())
    out_specs = P(None, "chan", None, "tm")

    def run(voltages, taps, busy_mask, drift_low):
        body = paired_shards if two_devices_hold_a_step(mesh, voltages) else shards
        return jax.shard_map(
            body, mesh=mesh, in_specs=in_specs, out_specs=out_specs, check_vma=False
        )(voltages, taps, busy_mask, drift_low)

    return run
```
